32 devices in a mesh: gx: 4 (over x, core), gy: 4 (over z), gz: 2 (over y).
Axes of the slice: x: 2, y: 2, z: 4, core: 2. Of those that a mesh axis runs over, the one named last changes fastest.
Arguments:
- field: float32 [64, 1024, 256], P('gx', 'gy', 'gz'), may hold values from -6 to 6
- source: float32 [64, 1024, 256], P('gx', 'gy', 'gz'), may hold values from -6 to 6
Outputs:
- smoothed: float32 [64, 1024, 256], P('gx', 'gy', 'gz')
The draws below stay inside these ranges and needn't reach their ends.
All inputs are finite; a program needn't handle non-finite values.
Results may differ from the reference program's by a relative error of at most 0.00002.
Values sent between devices are 32-bit elements; how exact they have to be, the bound alone decides.
A program may use at most 64 MiB of HBM per device.

```python
import jax
import jax.numpy as jnp

SWEEPS = 3
NX = 64
NY = 1024
NZ = 256


def block_levels(key, shape, split, least, top_value):
    def one(position, parts):
        draws = jax.random.uniform(jax.random.fold_in(jax.random.fold_in(key, 6), position), (parts,), jnp.float32, least / len(split), top_value / len(split))
        return jnp.repeat(jnp.exp(draws), shape[position] // parts).reshape((-1,) + (1,) * (len(shape) - position - 1))

    loudness = one(*split[0])
    for cut in split[1:]:
        loudness = loudness * one(*cut)
    return loudness


def bell_draw(own_key, shape, spread, most, shards=(), held_as=jnp.bfloat16):
    entries = jax.random.normal(own_key, shape, jnp.float32) * spread
    if len(shards) > 0:
        entries = block_levels(own_key, shape, shards, -0.22, 0.18) * entries
    return jnp.clip(entries, min=-most, max=most).astype(held_as)


def setup_inputs(seed: int = 0) -> dict:
    key_of = jax.random.split(jax.random.key(seed), 3)
    field = bell_draw(key_of[0], (NX, NY, NZ), 1.0, 6.0, ((0, 4), (1, 4), (2, 2)), jnp.float32)
    source = bell_draw(key_of[1], (NX, NY, NZ), 1.0, 6.0, ((0, 4), (1, 4), (2, 2)), jnp.float32)
    return dict(field=field, source=source)


def relax(values, source, parity, colour):
    padded = jnp.pad(values, ((1, 1), (0, 0), (0, 0)))
    beside = padded[2:] + padded[:-2]
    beside = beside + jnp.roll(values, -1, 1) + jnp.roll(values, 1, 1)
    beside = beside + jnp.roll(values, -1, 2) + jnp.roll(values, 1, 2)
    return jnp.where(parity == colour, (source + beside) / 6.0, values)


def reference(field, source):
    nx, ny, nz = field.shape
    parity = (jnp.arange(nx, dtype=jnp.int32)[:, None, None] + jnp.arange(ny, dtype=jnp.int32)[None, :, None] + jnp.arange(nz, dtype=jnp.int32)[None, None, :]) % 2
    values = field
    for sweep in range(SWEEPS):
        values = relax(values, source, parity, 0)
        values = relax(values, source, parity, 1)
    return values
```

```python
import functools

import jax
import jax.numpy as jnp
from jax import lax
from jax.experimental import pallas as pl
from jax.experimental.pallas import tpu as pltpu
from jax.sharding import PartitionSpec as P

SWEEPS = 3
MESH = pl.DeviceIdType.MESH
GROUP = 8
PAD = 8
X_LO, X_HI, Y_LO, Y_HI, Z_LO, Z_HI = range(6)


def kernel(sizes, f_hbm, s_hbm, o_hbm, fv, sv, ov, x, src, comb, kb, kr, jb, jr, ib, ir, send, recv, fsem, ssem, osem):
    ngx, ngy, ngz = sizes
    planes, rows, cols = f_hbm.shape
    nm = planes // 2
    half = rows // 2
    per_plane = rows // 8
    rounds = 2 * SWEEPS
    gx, gy, gz = (lax.axis_index(a) for a in ("gx", "gy", "gz"))
    has_lo, has_hi = gx > 0, gx < ngx - 1
    one_z = ngz == 2
    y_lo, y_hi = lax.rem(gy + ngy - 1, ngy), lax.rem(gy + 1, ngy)
    z_lo, z_hi = lax.rem(gz + ngz - 1, ngz), lax.rem(gz + 1, ngz)
    order = [0, nm - 1] + list(range(1, nm - 1))

    def load(ref, to, sem, m):
        return pltpu.make_async_copy(ref.at[pl.ds(2 * m, 2)], to.at[pl.ds(2 * m, 2)], sem.at[m])

    for m in order:
        load(f_hbm, fv, fsem, m).start()
    for m in order:
        load(s_hbm, sv, ssem, m).start()

    barrier = pltpu.get_barrier_semaphore()

    def greet(device):
        pl.semaphore_signal(barrier, inc=1, device_id=device, device_id_type=MESH)

    @pl.when(has_lo)
    def _():
        greet({"gx": gx - 1})

    @pl.when(has_hi)
    def _():
        greet({"gx": gx + 1})

    ys = [y_lo] if ngy == 2 else [y_lo, y_hi]
    zs = [z_lo] if one_z else [z_lo, z_hi]
    for y in ys:
        greet({"gy": y})
    for z in zs:
        greet({"gz": z})

    row8 = lax.broadcasted_iota(jnp.int32, (8, cols), 0)
    lane = lax.broadcasted_iota(jnp.int32, (8, cols), 1)
    odd8 = lax.rem(row8 + lane, 2)
    pair8 = lax.div(lane, 2)
    odd3 = jnp.broadcast_to(odd8[None], (GROUP, 8, cols)) == 1
    first3 = jnp.broadcast_to(lane[None], (GROUP, 8, cols)) == 0
    last3 = jnp.broadcast_to(lane[None], (GROUP, 8, cols)) == cols - 1
    even_lane = lax.rem(lane, 2) == 0
    odd_lane_half = lax.rem(lax.broadcasted_iota(jnp.int32, (half, cols), 1), 2) == 1

    zero = jnp.zeros((rows, cols), jnp.float32)

    @pl.when(jnp.logical_not(has_lo))
    def _():
        for c in range(2):
            x[c, 0, pl.ds(PAD, rows), :] = zero

    @pl.when(jnp.logical_not(has_hi))
    def _():
        for c in range(2):
            x[c, nm + 1, pl.ds(PAD, rows), :] = zero

    def three(v):
        return v.reshape(GROUP, 8, cols)

    def flat(v):
        return v.reshape(GROUP * 8, cols)

    def pair(produce, store, a, members, pack_to):
        acc = jnp.zeros((8, cols), jnp.float32)
        for h, m in enumerate(members):
            for blk in range(per_plane // GROUP):
                start = blk * GROUP * 8
                y = produce(a, m, h * per_plane + blk * GROUP, start)
                store(m, start, y)
                if pack_to is not None:
                    for g in range(GROUP):
                        q = h * per_plane + blk * GROUP + g
                        acc = jnp.where(pair8 == q, pltpu.roll(y[g], (2 * q + 1) % cols, 1), acc)
        if pack_to is not None:
            pack_to[a] = acc

    def inner(produce, store, pack_to):
        def body(a, carry):
            pair(produce, store, a, (1 + 2 * a, 2 + 2 * a), pack_to)
            return carry

        lax.fori_loop(0, nm // 2 - 1, body, 0)

    def outer(produce, store, pack_to):
        pair(produce, store, nm // 2 - 1, (0, nm - 1), pack_to)

    def copy(src_ref, dst_ref, to, t, out_dir, in_dir):
        return pltpu.make_async_remote_copy(
            src_ref=src_ref, dst_ref=dst_ref, send_sem=send.at[out_dir, t], recv_sem=recv.at[in_dir, t],
            device_id=to, device_id_type=MESH,
        )

    def x_lo_copy(t):
        return copy(ib.at[0, t], ir.at[1, t], {"gx": gx - 1}, t, X_LO, X_HI)

    def x_hi_copy(t):
        return copy(ib.at[1, t], ir.at[0, t], {"gx": gx + 1}, t, X_HI, X_LO)

    def y_copies(t):
        return (
            copy(jb.at[0, t], jr.at[1, t], {"gy": y_lo}, t, Y_LO, Y_HI),
            copy(jb.at[1, t], jr.at[0, t], {"gy": y_hi}, t, Y_HI, Y_LO),
        )

    def z_copies(t):
        up = copy(kb.at[t], kr.at[0, t], {"gz": z_hi}, t, Z_HI, Z_LO)
        if one_z:
            return (up,)
        return (up, copy(kb.at[t], kr.at[1, t], {"gz": z_lo}, t, Z_LO, Z_HI))

    def face(c, side):
        m = 1 if side == 0 else nm
        even = x[c, m, pl.ds(PAD, half, stride=2), :]
        odd = x[c, m, pl.ds(PAD + 1, half, stride=2), :]
        wanted = c if side == 0 else 1 - c
        return jnp.where(odd_lane_half, even, odd) if wanted == 1 else jnp.where(odd_lane_half, odd, even)

    def send_x(c, t):
        @pl.when(has_lo)
        def _():
            ib[0, t] = face(c, 0)
            x_lo_copy(t).start()

        @pl.when(has_hi)
        def _():
            ib[1, t] = face(c, 1)
            x_hi_copy(t).start()

    def send_yz(c, t):
        for z in z_copies(t):
            z.start()
        for m in range(nm):
            jb[0, t, pl.ds(m, 1), :] = x[c, m + 1, pl.ds(PAD, 1), :]
            jb[1, t, pl.ds(m, 1), :] = x[c, m + 1, pl.ds(PAD + rows - 1, 1), :]
        for y in y_copies(t):
            y.start()

    def take_yz(c, t):
        for z in z_copies(t):
            z.wait_recv()
        for a in range(nm // 2):
            low = kr[0, t, a]
            high = low if one_z else kr[1, t, a]
            comb[t, a] = jnp.where(even_lane, pltpu.roll(high, cols - 1, 1), pltpu.roll(low, 1, 1))
        for y in y_copies(t):
            y.wait_recv()
        for m in range(nm):
            x[c, m + 1, pl.ds(PAD - 1, 1), :] = jr[0, t, pl.ds(m, 1), :]
            x[c, m + 1, pl.ds(PAD + rows, 1), :] = jr[1, t, pl.ds(m, 1), :]

    def take_x(c, t):
        @pl.when(has_lo)
        def _():
            x_hi_copy_in = copy(ib.at[1, t], ir.at[0, t], {"gx": gx - 1}, t, X_HI, X_LO)
            x_hi_copy_in.wait_recv()
            got = ir[0, t]
            x[c, 0, pl.ds(PAD, half, stride=2), :] = got
            x[c, 0, pl.ds(PAD + 1, half, stride=2), :] = got

        @pl.when(has_hi)
        def _():
            x_lo_copy_in = copy(ib.at[0, t], ir.at[1, t], {"gx": gx + 1}, t, X_LO, X_HI)
            x_lo_copy_in.wait_recv()
            got = ir[1, t]
            x[c, nm + 1, pl.ds(PAD, half, stride=2), :] = got
            x[c, nm + 1, pl.ds(PAD + 1, half, stride=2), :] = got

    def store_to(c):
        def store(m, start, y):
            x[c, m + 1, pl.ds(PAD + start, GROUP * 8), :] = flat(y)

        return store

    def black_of_field(a, m, q0, start):
        low = three(fv[2 * m, pl.ds(start, GROUP * 8), :])
        high = three(fv[2 * m + 1, pl.ds(start, GROUP * 8), :])
        return jnp.where(odd3, low, high)

    for m in (0, nm - 1):
        load(f_hbm, fv, fsem, m).wait()
    pl.semaphore_wait(barrier, len(ys) + len(zs) + has_lo.astype(jnp.int32) + has_hi.astype(jnp.int32))
    outer(black_of_field, store_to(1), kb.at[0])
    send_x(1, 0)
    for m in range(1, nm - 1):
        load(f_hbm, fv, fsem, m).wait()
    inner(black_of_field, store_to(1), kb.at[0])
    send_yz(1, 0)

    for m in order:
        load(s_hbm, sv, ssem, m).wait()

    def split_source(m, carry):
        for blk in range(per_plane // GROUP):
            rs = pl.ds(blk * GROUP * 8, GROUP * 8)
            low, high = three(sv[2 * m, rs, :]), three(sv[2 * m + 1, rs, :])
            src[0, m, rs, :] = flat(jnp.where(odd3, high, low))
            src[1, m, rs, :] = flat(jnp.where(odd3, low, high))
        return carry

    lax.fori_loop(0, nm, split_source, 0)

    def relax(c, t):
        d = 1 - c

        def produce(a, m, q0, start):
            rs = pl.ds(PAD + start, GROUP * 8)
            here = three(x[d, m + 1, rs, :])
            below, above = three(x[d, m, rs, :]), three(x[d, m + 2, rs, :])
            beside = jnp.where(odd3, above, below) if c == 0 else jnp.where(odd3, below, above)
            total = three(src[c, m, pl.ds(start, GROUP * 8), :]) + here + beside
            total = total + three(x[d, m + 1, pl.ds(PAD + start - 1, GROUP * 8), :])
            total = total + three(x[d, m + 1, pl.ds(PAD + start + 1, GROUP * 8), :])
            edges = comb[t, a]
            edge = jnp.stack(
                [pltpu.roll(edges, (2 * cols - (2 * (q0 + g) + 1)) % cols, 1) for g in range(GROUP)], axis=0
            )
            total = total + jnp.where(first3, edge, pltpu.roll(here, 1, 2))
            total = total + jnp.where(last3, edge, pltpu.roll(here, cols - 1, 2))
            return total * jnp.float32(1.0 / 6.0)

        return produce

    def out_copy(m):
        return pltpu.make_async_copy(ov.at[pl.ds(2 * m, 2)], o_hbm.at[pl.ds(2 * m, 2)], osem.at[m])

    def store_out(m, start, y):
        red = three(x[0, m + 1, pl.ds(PAD + start, GROUP * 8), :])
        rs = pl.ds(start, GROUP * 8)
        ov[2 * m, rs, :] = flat(jnp.where(odd3, y, red))
        ov[2 * m + 1, rs, :] = flat(jnp.where(odd3, red, y))

    for t in range(rounds):
        c = t % 2
        final = t == rounds - 1
        store = store_out if final else store_to(c)
        pack = None if final else kb.at[t + 1]
        take_yz(1 - c, t)
        inner(relax(c, t), store, pack)
        if final:
            for m in range(1, nm - 1):
                out_copy(m).start()
        take_x(1 - c, t)
        outer(relax(c, t), store, pack)
        if final:
            for m in (0, nm - 1):
                out_copy(m).start()
        else:
            send_x(c, t + 1)
            send_yz(c, t + 1)

    for t in range(rounds):
        for cp in z_copies(t) + y_copies(t):
            cp.wait_send()

        @pl.when(has_lo)
        def _():
            x_lo_copy(t).wait_send()

        @pl.when(has_hi)
        def _():
            x_hi_copy(t).wait_send()

    for m in range(nm):
        out_copy(m).wait()


def solution(mesh):
    sizes = tuple(mesh.shape[a] for a in ("gx", "gy", "gz"))

    def on_device(field, source):
        planes, rows, cols = field.shape
        nm, rounds = planes // 2, 2 * SWEEPS
        assert planes % 4 == 0 and rows % (8 * GROUP) == 0 and cols == 128 and rows // 2 == cols
        f32 = jnp.float32
        return pl.pallas_call(
            functools.partial(kernel, sizes),
            out_shape=jax.ShapeDtypeStruct(field.shape, f32),
            in_specs=[pl.BlockSpec(memory_space=pl.ANY)] * 2,
            out_specs=pl.BlockSpec(memory_space=pl.ANY),
            scratch_shapes=[
                pltpu.VMEM(field.shape, f32),
                pltpu.VMEM(field.shape, f32),
                pltpu.VMEM(field.shape, f32),
                pltpu.VMEM((2, nm + 2, rows + 2 * PAD, cols), f32),
                pltpu.VMEM((2, nm, rows, cols), f32),
                pltpu.VMEM((rounds, nm // 2, 8, cols), f32),
                pltpu.VMEM((rounds, nm // 2, 8, cols), f32),
                pltpu.VMEM((2, rounds, nm // 2, 8, cols), f32),
                pltpu.VMEM((2, rounds, nm, cols), f32),
                pltpu.VMEM((2, rounds, nm, cols), f32),
                pltpu.VMEM((2, rounds, rows // 2, cols), f32),
                pltpu.VMEM((2, rounds, rows // 2, cols), f32),
                pltpu.SemaphoreType.DMA((6, rounds)),
                pltpu.SemaphoreType.DMA((6, rounds)),
                pltpu.SemaphoreType.DMA((nm,)),
                pltpu.SemaphoreType.DMA((nm,)),
                pltpu.SemaphoreType.DMA((nm,)),
            ],
            compiler_params=pltpu.CompilerParams(
                collective_id=0, has_side_effects=True, vmem_limit_bytes=32 * 1024 * 1024
            ),
        )(field, source)

    spec = P("gx", "gy", "gz")
    return jax.shard_map(on_device, mesh=mesh, in_specs=(spec, spec), out_specs=spec, check_vma=False)
```

```python
import functools

import jax
import jax.numpy as jnp
from jax import lax
from jax.experimental import pallas as pl
from jax.experimental.pallas import tpu as pltpu
from jax.sharding import PartitionSpec as P

SWEEPS = 3
MESH = pl.DeviceIdType.MESH
GROUP = 8
PAD = 8
X_LO, X_HI, Y_LO, Y_HI, Z_LO, Z_HI = range(6)


def kernel(sizes, f_hbm, s_hbm, ov, fv, sv, x, src, comb, kb, kr, jb, jr, ib, ir, send, recv, fsem, ssem):
    ngx, ngy, ngz = sizes
    planes, rows, cols = f_hbm.shape
    nm = planes // 2
    half = rows // 2
    per_plane = rows // 8
    rounds = 2 * SWEEPS
    gx, gy, gz = (lax.axis_index(a) for a in ("gx", "gy", "gz"))
    has_lo, has_hi = gx > 0, gx < ngx - 1
    one_z = ngz == 2
    y_lo, y_hi = lax.rem(gy + ngy - 1, ngy), lax.rem(gy + 1, ngy)
    z_lo, z_hi = lax.rem(gz + ngz - 1, ngz), lax.rem(gz + 1, ngz)
    order = [0, nm - 1] + list(range(1, nm - 1))

    def load(ref, to, sem, m):
        return pltpu.make_async_copy(ref.at[pl.ds(2 * m, 2)], to.at[pl.ds(2 * m, 2)], sem.at[m])

    for m in order:
        load(f_hbm, fv, fsem, m).start()
    for m in order:
        load(s_hbm, sv, ssem, m).start()

    barrier = pltpu.get_barrier_semaphore()

    def greet(device):
        pl.semaphore_signal(barrier, inc=1, device_id=device, device_id_type=MESH)

    @pl.when(has_lo)
    def _():
        greet({"gx": gx - 1})

    @pl.when(has_hi)
    def _():
        greet({"gx": gx + 1})

    ys = [y_lo] if ngy == 2 else [y_lo, y_hi]
    zs = [z_lo] if one_z else [z_lo, z_hi]
    for y in ys:
        greet({"gy": y})
    for z in zs:
        greet({"gz": z})

    row8 = lax.broadcasted_iota(jnp.int32, (8, cols), 0)
    lane = lax.broadcasted_iota(jnp.int32, (8, cols), 1)
    odd8 = lax.rem(row8 + lane, 2)
    pair8 = lax.div(lane, 2)
    odd3 = jnp.broadcast_to(odd8[None], (GROUP, 8, cols)) == 1
    first3 = jnp.broadcast_to(lane[None], (GROUP, 8, cols)) == 0
    last3 = jnp.broadcast_to(lane[None], (GROUP, 8, cols)) == cols - 1
    even_lane = lax.rem(lane, 2) == 0
    odd_lane_half = lax.rem(lax.broadcasted_iota(jnp.int32, (half, cols), 1), 2) == 1

    zero = jnp.zeros((rows, cols), jnp.float32)

    @pl.when(jnp.logical_not(has_lo))
    def _():
        for c in range(2):
            x[c, 0, pl.ds(PAD, rows), :] = zero

    @pl.when(jnp.logical_not(has_hi))
    def _():
        for c in range(2):
            x[c, nm + 1, pl.ds(PAD, rows), :] = zero

    def three(v):
        return v.reshape(GROUP, 8, cols)

    def flat(v):
        return v.reshape(GROUP * 8, cols)

    def pair(produce, store, a, pack_to):
        accs = []
        for h, m in enumerate((a, nm - 1 - a)):
            for blk in range(per_plane // GROUP):
                start = blk * GROUP * 8
                y = produce(a, m, h * per_plane + blk * GROUP, start)
                store(m, start, y)
                if pack_to is not None:
                    acc = jnp.zeros((8, cols), jnp.float32)
                    for g in range(GROUP):
                        q = h * per_plane + blk * GROUP + g
                        acc = jnp.where(pair8 == q, pltpu.roll(y[g], (2 * q + 1) % cols, 1), acc)
                    accs.append(acc)
        if pack_to is not None:
            while len(accs) > 1:
                accs = [p + q for p, q in zip(accs[::2], accs[1::2])]
            pack_to[a] = accs[0]

    def copy(src_ref, dst_ref, to, at, out_dir, in_dir):
        return pltpu.make_async_remote_copy(
            src_ref=src_ref, dst_ref=dst_ref, send_sem=send.at[(out_dir, *at)], recv_sem=recv.at[(in_dir, *at)],
            device_id=to, device_id_type=MESH,
        )

    def x_lo_copy(t):
        return copy(ib.at[0, t], ir.at[1, t], {"gx": gx - 1}, (t, 0), X_LO, X_HI)

    def x_hi_copy(t):
        return copy(ib.at[1, t], ir.at[0, t], {"gx": gx + 1}, (t, 0), X_HI, X_LO)

    def y_copies(t, a):
        return (
            copy(jb.at[0, t, a], jr.at[1, t, a], {"gy": y_lo}, (t, a), Y_LO, Y_HI),
            copy(jb.at[1, t, a], jr.at[0, t, a], {"gy": y_hi}, (t, a), Y_HI, Y_LO),
        )

    def z_copies(t, a):
        up = copy(kb.at[t, a], kr.at[0, t, a], {"gz": z_hi}, (t, a), Z_HI, Z_LO)
        if one_z:
            return (up,)
        return (up, copy(kb.at[t, a], kr.at[1, t, a], {"gz": z_lo}, (t, a), Z_LO, Z_HI))

    def face(c, side):
        m = 1 if side == 0 else nm
        even = x[c, m, pl.ds(PAD, half, stride=2), :]
        odd = x[c, m, pl.ds(PAD + 1, half, stride=2), :]
        wanted = c if side == 0 else 1 - c
        return jnp.where(odd_lane_half, even, odd) if wanted == 1 else jnp.where(odd_lane_half, odd, even)

    def send_x(c, t):
        @pl.when(has_lo)
        def _():
            ib[0, t] = face(c, 0)
            x_lo_copy(t).start()

        @pl.when(has_hi)
        def _():
            ib[1, t] = face(c, 1)
            x_hi_copy(t).start()

    def send_yz(c, t, a):
        for z in z_copies(t, a):
            z.start()
        for h, m in enumerate((a, nm - 1 - a)):
            jb[0, t, a, pl.ds(h, 1), :] = x[c, m + 1, pl.ds(PAD, 1), :]
            jb[1, t, a, pl.ds(h, 1), :] = x[c, m + 1, pl.ds(PAD + rows - 1, 1), :]
        for y in y_copies(t, a):
            y.start()

    def take_yz(c, t, a):
        for z in z_copies(t, a):
            z.wait_recv()
        low = kr[0, t, a]
        high = low if one_z else kr[1, t, a]
        comb[a] = jnp.where(even_lane, pltpu.roll(high, cols - 1, 1), pltpu.roll(low, 1, 1))
        for y in y_copies(t, a):
            y.wait_recv()
        for h, m in enumerate((a, nm - 1 - a)):
            x[c, m + 1, pl.ds(PAD - 1, 1), :] = jr[0, t, a, pl.ds(h, 1), :]
            x[c, m + 1, pl.ds(PAD + rows, 1), :] = jr[1, t, a, pl.ds(h, 1), :]

    def take_x(c, t):
        @pl.when(has_lo)
        def _():
            x_hi_copy_in = copy(ib.at[1, t], ir.at[0, t], {"gx": gx - 1}, (t, 0), X_HI, X_LO)
            x_hi_copy_in.wait_recv()
            got = ir[0, t]
            x[c, 0, pl.ds(PAD, half, stride=2), :] = got
            x[c, 0, pl.ds(PAD + 1, half, stride=2), :] = got

        @pl.when(has_hi)
        def _():
            x_lo_copy_in = copy(ib.at[0, t], ir.at[1, t], {"gx": gx + 1}, (t, 0), X_LO, X_HI)
            x_lo_copy_in.wait_recv()
            got = ir[1, t]
            x[c, nm + 1, pl.ds(PAD, half, stride=2), :] = got
            x[c, nm + 1, pl.ds(PAD + 1, half, stride=2), :] = got

    def store_to(c):
        def store(m, start, y):
            x[c, m + 1, pl.ds(PAD + start, GROUP * 8), :] = flat(y)

        return store

    def black_of_field(a, m, q0, start):
        low = three(fv[2 * m, pl.ds(start, GROUP * 8), :])
        high = three(fv[2 * m + 1, pl.ds(start, GROUP * 8), :])
        return jnp.where(odd3, low, high)

    for m in (0, nm - 1):
        load(f_hbm, fv, fsem, m).wait()
    pl.semaphore_wait(barrier, len(ys) + len(zs) + has_lo.astype(jnp.int32) + has_hi.astype(jnp.int32))
    pair(black_of_field, store_to(1), 0, kb.at[0])
    send_x(1, 0)
    send_yz(1, 0, 0)

    def first(a, carry):
        for m in (a, nm - 1 - a):
            load(f_hbm, fv, fsem, m).wait()
        pair(black_of_field, store_to(1), a, kb.at[0])
        send_yz(1, 0, a)
        return carry

    lax.fori_loop(1, nm // 2, first, 0)

    for m in order:
        load(s_hbm, sv, ssem, m).wait()

    def split_source(m, carry):
        for blk in range(per_plane // GROUP):
            rs = pl.ds(blk * GROUP * 8, GROUP * 8)
            low, high = three(sv[2 * m, rs, :]), three(sv[2 * m + 1, rs, :])
            src[0, m, rs, :] = flat(jnp.where(odd3, high, low))
            src[1, m, rs, :] = flat(jnp.where(odd3, low, high))
        return carry

    lax.fori_loop(0, nm, split_source, 0)

    def relax(c, t):
        d = 1 - c

        def produce(a, m, q0, start):
            rs = pl.ds(PAD + start, GROUP * 8)
            here = three(x[d, m + 1, rs, :])
            below, above = three(x[d, m, rs, :]), three(x[d, m + 2, rs, :])
            beside = jnp.where(odd3, above, below) if c == 0 else jnp.where(odd3, below, above)
            total = three(src[c, m, pl.ds(start, GROUP * 8), :]) + here + beside
            total = total + three(x[d, m + 1, pl.ds(PAD + start - 1, GROUP * 8), :])
            total = total + three(x[d, m + 1, pl.ds(PAD + start + 1, GROUP * 8), :])
            edges = comb[a]
            edge = jnp.stack(
                [pltpu.roll(edges, (2 * cols - (2 * (q0 + g) + 1)) % cols, 1) for g in range(GROUP)], axis=0
            )
            total = total + jnp.where(first3, edge, pltpu.roll(here, 1, 2))
            total = total + jnp.where(last3, edge, pltpu.roll(here, cols - 1, 2))
            return total * jnp.float32(1.0 / 6.0)

        return produce

    def store_out(m, start, y):
        red = three(x[0, m + 1, pl.ds(PAD + start, GROUP * 8), :])
        rs = pl.ds(start, GROUP * 8)
        ov[2 * m, rs, :] = flat(jnp.where(odd3, y, red))
        ov[2 * m + 1, rs, :] = flat(jnp.where(odd3, red, y))

    for t in range(rounds):
        c = t % 2
        final = t == rounds - 1
        store = store_out if final else store_to(c)
        pack = None if final else kb.at[t + 1]

        def piece(a, first=False):
            take_yz(1 - c, t, a)
            if first:
                take_x(1 - c, t)
            pair(relax(c, t), store, a, pack)
            if not final:
                if first:
                    send_x(c, t + 1)
                send_yz(c, t + 1, a)

        def body(a, carry):
            piece(a)
            return carry

        piece(0, True)
        lax.fori_loop(1, nm // 2, body, 0)

    for t in range(rounds):
        for a in range(nm // 2):
            for cp in z_copies(t, a) + y_copies(t, a):
                cp.wait_send()

        @pl.when(has_lo)
        def _():
            x_lo_copy(t).wait_send()

        @pl.when(has_hi)
        def _():
            x_hi_copy(t).wait_send()


def solution(mesh):
    sizes = tuple(mesh.shape[a] for a in ("gx", "gy", "gz"))

    def on_device(field, source):
        planes, rows, cols = field.shape
        nm, rounds = planes // 2, 2 * SWEEPS
        assert planes % 4 == 0 and rows % (8 * GROUP) == 0 and cols == 128 and rows // 2 == cols
        f32 = jnp.float32
        return pl.pallas_call(
            functools.partial(kernel, sizes),
            out_shape=jax.ShapeDtypeStruct(field.shape, f32),
            in_specs=[pl.BlockSpec(memory_space=pltpu.HBM)] * 2,
            out_specs=pl.BlockSpec(memory_space=pltpu.VMEM),
            scratch_shapes=[
                pltpu.VMEM(field.shape, f32),
                pltpu.VMEM(field.shape, f32),
                pltpu.VMEM((2, nm + 2, rows + 2 * PAD, cols), f32),
                pltpu.VMEM((2, nm, rows, cols), f32),
                pltpu.VMEM((nm // 2, 8, cols), f32),
                pltpu.VMEM((rounds, nm // 2, 8, cols), f32),
                pltpu.VMEM((2, rounds, nm // 2, 8, cols), f32),
                pltpu.VMEM((2, rounds, nm // 2, 2, cols), f32),
                pltpu.VMEM((2, rounds, nm // 2, 2, cols), f32),
                pltpu.VMEM((2, rounds, rows // 2, cols), f32),
                pltpu.VMEM((2, rounds, rows // 2, cols), f32),
                pltpu.SemaphoreType.DMA((6, rounds, nm // 2)),
                pltpu.SemaphoreType.DMA((6, rounds, nm // 2)),
                pltpu.SemaphoreType.DMA((nm,)),
                pltpu.SemaphoreType.DMA((nm,)),
            ],
            compiler_params=pltpu.CompilerParams(
                collective_id=0, has_side_effects=True, vmem_limit_bytes=60 * 1024 * 1024
            ),
        )(field, source)

    spec = P("gx", "gy", "gz")
    return jax.shard_map(on_device, mesh=mesh, in_specs=(spec, spec), out_specs=spec, check_vma=False)
```

```python
import functools

import jax
import jax.numpy as jnp
from jax import lax
from jax.experimental import pallas as pl
from jax.experimental.pallas import tpu as pltpu
from jax.sharding import PartitionSpec as P

SWEEPS = 3
MESH = pl.DeviceIdType.MESH
GROUP = 32
PAD = 8
X_LO, X_HI, Y_LO, Y_HI, Z_LO, Z_HI = range(6)


def kernel(sizes, f_hbm, s_hbm, ov, fv, sv, x, src, comb, kb, kr, jb, jr, ib, ir, send, recv, fsem, ssem):
    ngx, ngy, ngz = sizes
    planes, rows, cols = f_hbm.shape
    nm = planes // 2
    half = rows // 2
    per_plane = rows // 8
    rounds = 2 * SWEEPS
    gx, gy, gz = (lax.axis_index(a) for a in ("gx", "gy", "gz"))
    has_lo, has_hi = gx > 0, gx < ngx - 1
    one_z = ngz == 2
    y_lo, y_hi = lax.rem(gy + ngy - 1, ngy), lax.rem(gy + 1, ngy)
    z_lo, z_hi = lax.rem(gz + ngz - 1, ngz), lax.rem(gz + 1, ngz)
    order = [m for a in range(nm // 2) for m in (a, nm - 1 - a)]

    def load(ref, to, sem, m):
        return pltpu.make_async_copy(ref.at[pl.ds(2 * m, 2)], to.at[pl.ds(2 * m, 2)], sem.at[m])

    for m in order:
        load(f_hbm, fv, fsem, m).start()
    for m in order:
        load(s_hbm, sv, ssem, m).start()

    barrier = pltpu.get_barrier_semaphore()

    def greet(device):
        pl.semaphore_signal(barrier, inc=1, device_id=device, device_id_type=MESH)

    @pl.when(has_lo)
    def _():
        greet({"gx": gx - 1})

    @pl.when(has_hi)
    def _():
        greet({"gx": gx + 1})

    ys = [y_lo] if ngy == 2 else [y_lo, y_hi]
    zs = [z_lo] if one_z else [z_lo, z_hi]
    for y in ys:
        greet({"gy": y})
    for z in zs:
        greet({"gz": z})

    row8 = lax.broadcasted_iota(jnp.int32, (8, cols), 0)
    lane = lax.broadcasted_iota(jnp.int32, (8, cols), 1)
    odd8 = lax.rem(row8 + lane, 2)
    pair8 = lax.div(lane, 2)
    odd3 = jnp.broadcast_to(odd8[None], (GROUP, 8, cols)) == 1
    first3 = jnp.broadcast_to(lane[None], (GROUP, 8, cols)) == 0
    last3 = jnp.broadcast_to(lane[None], (GROUP, 8, cols)) == cols - 1
    even_lane = lax.rem(lane, 2) == 0
    odd_lane_half = lax.rem(lax.broadcasted_iota(jnp.int32, (half, cols), 1), 2) == 1

    zero = jnp.zeros((rows, cols), jnp.float32)

    @pl.when(jnp.logical_not(has_lo))
    def _():
        for c in range(2):
            x[c, 0, pl.ds(PAD, rows), :] = zero

    @pl.when(jnp.logical_not(has_hi))
    def _():
        for c in range(2):
            x[c, nm + 1, pl.ds(PAD, rows), :] = zero

    def three(v):
        return v.reshape(GROUP, 8, cols)

    def flat(v):
        return v.reshape(GROUP * 8, cols)

    def pair(produce, store, a, pack_to):
        accs = []
        for h, m in enumerate((a, nm - 1 - a)):
            for blk in range(per_plane // GROUP):
                start = blk * GROUP * 8
                y = produce(a, m, h * per_plane + blk * GROUP, start)
                store(m, start, y)
                if pack_to is not None:
                    acc = jnp.zeros((8, cols), jnp.float32)
                    for g in range(GROUP):
                        q = h * per_plane + blk * GROUP + g
                        acc = jnp.where(pair8 == q, pltpu.roll(y[g], (2 * q + 1) % cols, 1), acc)
                    accs.append(acc)
        if pack_to is not None:
            while len(accs) > 1:
                accs = [p + q for p, q in zip(accs[::2], accs[1::2])]
            pack_to[a] = accs[0]

    def copy(src_ref, dst_ref, to, at, out_dir, in_dir):
        return pltpu.make_async_remote_copy(
            src_ref=src_ref, dst_ref=dst_ref, send_sem=send.at[(out_dir, *at)], recv_sem=recv.at[(in_dir, *at)],
            device_id=to, device_id_type=MESH,
        )

    def x_lo_copy(t):
        return copy(ib.at[0, t], ir.at[1, t], {"gx": gx - 1}, (t, 0), X_LO, X_HI)

    def x_hi_copy(t):
        return copy(ib.at[1, t], ir.at[0, t], {"gx": gx + 1}, (t, 0), X_HI, X_LO)

    def y_copies(t, a):
        return (
            copy(jb.at[0, t, a], jr.at[1, t, a], {"gy": y_lo}, (t, a), Y_LO, Y_HI),
            copy(jb.at[1, t, a], jr.at[0, t, a], {"gy": y_hi}, (t, a), Y_HI, Y_LO),
        )

    def z_copies(t, a):
        up = copy(kb.at[t, a], kr.at[0, t, a], {"gz": z_hi}, (t, a), Z_HI, Z_LO)
        if one_z:
            return (up,)
        return (up, copy(kb.at[t, a], kr.at[1, t, a], {"gz": z_lo}, (t, a), Z_LO, Z_HI))

    def face(c, side):
        m = 1 if side == 0 else nm
        even = x[c, m, pl.ds(PAD, half, stride=2), :]
        odd = x[c, m, pl.ds(PAD + 1, half, stride=2), :]
        wanted = c if side == 0 else 1 - c
        return jnp.where(odd_lane_half, even, odd) if wanted == 1 else jnp.where(odd_lane_half, odd, even)

    def send_x(c, t):
        @pl.when(has_lo)
        def _():
            ib[0, t] = face(c, 0)
            x_lo_copy(t).start()

        @pl.when(has_hi)
        def _():
            ib[1, t] = face(c, 1)
            x_hi_copy(t).start()

    def send_yz(c, t, a):
        for z in z_copies(t, a):
            z.start()
        for h, m in enumerate((a, nm - 1 - a)):
            jb[0, t, a, pl.ds(h, 1), :] = x[c, m + 1, pl.ds(PAD, 1), :]
            jb[1, t, a, pl.ds(h, 1), :] = x[c, m + 1, pl.ds(PAD + rows - 1, 1), :]
        for y in y_copies(t, a):
            y.start()

    def take_yz(c, t, a):
        for z in z_copies(t, a):
            z.wait_recv()
        low = kr[0, t, a]
        high = low if one_z else kr[1, t, a]
        comb[a] = jnp.where(even_lane, pltpu.roll(high, cols - 1, 1), pltpu.roll(low, 1, 1))
        for y in y_copies(t, a):
            y.wait_recv()
        for h, m in enumerate((a, nm - 1 - a)):
            x[c, m + 1, pl.ds(PAD - 1, 1), :] = jr[0, t, a, pl.ds(h, 1), :]
            x[c, m + 1, pl.ds(PAD + rows, 1), :] = jr[1, t, a, pl.ds(h, 1), :]

    def take_x(c, t):
        @pl.when(has_lo)
        def _():
            x_hi_copy_in = copy(ib.at[1, t], ir.at[0, t], {"gx": gx - 1}, (t, 0), X_HI, X_LO)
            x_hi_copy_in.wait_recv()
            got = ir[0, t]
            x[c, 0, pl.ds(PAD, half, stride=2), :] = got
            x[c, 0, pl.ds(PAD + 1, half, stride=2), :] = got

        @pl.when(has_hi)
        def _():
            x_lo_copy_in = copy(ib.at[0, t], ir.at[1, t], {"gx": gx + 1}, (t, 0), X_LO, X_HI)
            x_lo_copy_in.wait_recv()
            got = ir[1, t]
            x[c, nm + 1, pl.ds(PAD, half, stride=2), :] = got
            x[c, nm + 1, pl.ds(PAD + 1, half, stride=2), :] = got

    def store_to(c):
        def store(m, start, y):
            x[c, m + 1, pl.ds(PAD + start, GROUP * 8), :] = flat(y)

        return store

    def black_of_field(a, m, q0, start):
        low = three(fv[2 * m, pl.ds(start, GROUP * 8), :])
        high = three(fv[2 * m + 1, pl.ds(start, GROUP * 8), :])
        return jnp.where(odd3, low, high)

    def pack_field(a, carry):
        for m in (a, nm - 1 - a):
            load(f_hbm, fv, fsem, m).wait()
        pair(black_of_field, store_to(1), a, kb.at[0])
        return carry

    def split_source(m, carry):
        for blk in range(per_plane // GROUP):
            rs = pl.ds(blk * GROUP * 8, GROUP * 8)
            low, high = three(sv[2 * m, rs, :]), three(sv[2 * m + 1, rs, :])
            src[0, m, rs, :] = flat(jnp.where(odd3, high, low))
            src[1, m, rs, :] = flat(jnp.where(odd3, low, high))
        return carry

    def split_pair(a, carry):
        for m in (a, nm - 1 - a):
            load(s_hbm, sv, ssem, m).wait()
            split_source(m, 0)
        return carry

    lax.fori_loop(0, nm // 2, pack_field, 0)
    lax.fori_loop(0, nm // 2, split_pair, 0)
    pl.semaphore_wait(barrier, len(ys) + len(zs) + has_lo.astype(jnp.int32) + has_hi.astype(jnp.int32))
    send_x(1, 0)
    for a in range(nm // 2):
        send_yz(1, 0, a)

    def relax(c, t):
        d = 1 - c

        def produce(a, m, q0, start):
            rs = pl.ds(PAD + start, GROUP * 8)
            here = three(x[d, m + 1, rs, :])
            below, above = three(x[d, m, rs, :]), three(x[d, m + 2, rs, :])
            beside = jnp.where(odd3, above, below) if c == 0 else jnp.where(odd3, below, above)
            total = three(src[c, m, pl.ds(start, GROUP * 8), :]) + here + beside
            total = total + three(x[d, m + 1, pl.ds(PAD + start - 1, GROUP * 8), :])
            total = total + three(x[d, m + 1, pl.ds(PAD + start + 1, GROUP * 8), :])
            edges = comb[a]
            edge = jnp.stack(
                [pltpu.roll(edges, (2 * cols - (2 * (q0 + g) + 1)) % cols, 1) for g in range(GROUP)], axis=0
            )
            total = total + jnp.where(first3, edge, pltpu.roll(here, 1, 2))
            total = total + jnp.where(last3, edge, pltpu.roll(here, cols - 1, 2))
            return total * jnp.float32(1.0 / 6.0)

        return produce

    def store_out(m, start, y):
        red = three(x[0, m + 1, pl.ds(PAD + start, GROUP * 8), :])
        rs = pl.ds(start, GROUP * 8)
        ov[2 * m, rs, :] = flat(jnp.where(odd3, y, red))
        ov[2 * m + 1, rs, :] = flat(jnp.where(odd3, red, y))

    for t in range(rounds):
        c = t % 2
        final = t == rounds - 1
        store = store_out if final else store_to(c)
        pack = None if final else kb.at[t + 1]

        def piece(a, first=False):
            take_yz(1 - c, t, a)
            if first:
                take_x(1 - c, t)
            pair(relax(c, t), store, a, pack)
            if not final:
                if first:
                    send_x(c, t + 1)
                send_yz(c, t + 1, a)

        def body(a, carry):
            piece(a)
            return carry

        piece(0, True)
        lax.fori_loop(1, nm // 2, body, 0)

    for t in range(rounds):
        for a in range(nm // 2):
            for cp in z_copies(t, a) + y_copies(t, a):
                cp.wait_send()

        @pl.when(has_lo)
        def _():
            x_lo_copy(t).wait_send()

        @pl.when(has_hi)
        def _():
            x_hi_copy(t).wait_send()


def solution(mesh):
    sizes = tuple(mesh.shape[a] for a in ("gx", "gy", "gz"))

    def on_device(field, source):
        planes, rows, cols = field.shape
        nm, rounds = planes // 2, 2 * SWEEPS
        assert planes % 4 == 0 and rows % (8 * GROUP) == 0 and cols == 128 and rows // 2 == cols
        f32 = jnp.float32
        return pl.pallas_call(
            functools.partial(kernel, sizes),
            out_shape=jax.ShapeDtypeStruct(field.shape, f32),
            in_specs=[pl.BlockSpec(memory_space=pltpu.HBM)] * 2,
            out_specs=pl.BlockSpec(memory_space=pltpu.VMEM),
            scratch_shapes=[
                pltpu.VMEM(field.shape, f32),
                pltpu.VMEM(field.shape, f32),
                pltpu.VMEM((2, nm + 2, rows + 2 * PAD, cols), f32),
                pltpu.VMEM((2, nm, rows, cols), f32),
                pltpu.VMEM((nm // 2, 8, cols), f32),
                pltpu.VMEM((rounds, nm // 2, 8, cols), f32),
                pltpu.VMEM((2, rounds, nm // 2, 8, cols), f32),
                pltpu.VMEM((2, rounds, nm // 2, 2, cols), f32),
                pltpu.VMEM((2, rounds, nm // 2, 2, cols), f32),
                pltpu.VMEM((2, rounds, rows // 2, cols), f32),
                pltpu.VMEM((2, rounds, rows // 2, cols), f32),
                pltpu.SemaphoreType.DMA((6, rounds, nm // 2)),
                pltpu.SemaphoreType.DMA((6, rounds, nm // 2)),
                pltpu.SemaphoreType.DMA((nm,)),
                pltpu.SemaphoreType.DMA((nm,)),
            ],
            compiler_params=pltpu.CompilerParams(
                collective_id=0, has_side_effects=True, vmem_limit_bytes=50 * 1024 * 1024
            ),
        )(field, source)

    spec = P("gx", "gy", "gz")
    return jax.shard_map(on_device, mesh=mesh, in_specs=(spec, spec), out_specs=spec, check_vma=False)
```

```python
import functools

import jax
import jax.numpy as jnp
from jax import lax
from jax.experimental import pallas as pl
from jax.experimental.pallas import tpu as pltpu
from jax.sharding import PartitionSpec as P

SWEEPS = 3
MESH = pl.DeviceIdType.MESH
GROUP = 32
PAD = 8
X_LO, X_HI, Y_LO, Y_HI, Z_LO, Z_HI = range(6)


def kernel(sizes, f_hbm, s_hbm, ov, fv, sv, x, src, comb, kb, kr, jb, jr, ib, ir, send, recv, fsem, ssem):
    ngx, ngy, ngz = sizes
    planes, rows, cols = f_hbm.shape
    nm = planes // 2
    half = rows // 2
    per_plane = rows // 8
    rounds = 2 * SWEEPS
    gx, gy, gz = (lax.axis_index(a) for a in ("gx", "gy", "gz"))
    has_lo, has_hi = gx > 0, gx < ngx - 1
    one_z = ngz == 2
    y_lo, y_hi = lax.rem(gy + ngy - 1, ngy), lax.rem(gy + 1, ngy)
    z_lo, z_hi = lax.rem(gz + ngz - 1, ngz), lax.rem(gz + 1, ngz)
    order = [m for a in range(nm // 2) for m in (a, nm - 1 - a)]

    def load(ref, to, sem, m):
        return pltpu.make_async_copy(ref.at[pl.ds(2 * m, 2)], to.at[pl.ds(2 * m, 2)], sem.at[m])

    for m in order:
        load(f_hbm, fv, fsem, m).start()
    for m in order:
        load(s_hbm, sv, ssem, m).start()

    barrier = pltpu.get_barrier_semaphore()

    def greet(device):
        pl.semaphore_signal(barrier, inc=1, device_id=device, device_id_type=MESH)

    @pl.when(has_lo)
    def _():
        greet({"gx": gx - 1})

    @pl.when(has_hi)
    def _():
        greet({"gx": gx + 1})

    ys = [y_lo] if ngy == 2 else [y_lo, y_hi]
    zs = [z_lo] if one_z else [z_lo, z_hi]
    for y in ys:
        greet({"gy": y})
    for z in zs:
        greet({"gz": z})

    row8 = lax.broadcasted_iota(jnp.int32, (8, cols), 0)
    lane = lax.broadcasted_iota(jnp.int32, (8, cols), 1)
    odd8 = lax.rem(row8 + lane, 2)
    pair8 = lax.div(lane, 2)
    odd3 = jnp.broadcast_to(odd8[None], (GROUP, 8, cols)) == 1
    first3 = jnp.broadcast_to(lane[None], (GROUP, 8, cols)) == 0
    last3 = jnp.broadcast_to(lane[None], (GROUP, 8, cols)) == cols - 1
    even_lane = lax.rem(lane, 2) == 0
    odd_lane_half = lax.rem(lax.broadcasted_iota(jnp.int32, (half, cols), 1), 2) == 1

    zero = jnp.zeros((rows, cols), jnp.float32)

    @pl.when(jnp.logical_not(has_lo))
    def _():
        for c in range(2):
            x[c, 0, pl.ds(PAD, rows), :] = zero

    @pl.when(jnp.logical_not(has_hi))
    def _():
        for c in range(2):
            x[c, nm + 1, pl.ds(PAD, rows), :] = zero

    def three(v):
        return v.reshape(GROUP, 8, cols)

    def flat(v):
        return v.reshape(GROUP * 8, cols)

    def pair(produce, store, a, pack_to):
        accs = []
        for h, m in enumerate((a, nm - 1 - a)):
            for blk in range(per_plane // GROUP):
                start = blk * GROUP * 8
                y = produce(a, m, h * per_plane + blk * GROUP, start)
                store(m, start, y)
                if pack_to is not None:
                    acc = jnp.zeros((8, cols), jnp.float32)
                    for g in range(GROUP):
                        q = h * per_plane + blk * GROUP + g
                        acc = jnp.where(pair8 == q, pltpu.roll(y[g], (2 * q + 1) % cols, 1), acc)
                    accs.append(acc)
        if pack_to is not None:
            while len(accs) > 1:
                accs = [p + q for p, q in zip(accs[::2], accs[1::2])]
            pack_to[a] = accs[0]

    def copy(src_ref, dst_ref, to, at, out_dir, in_dir):
        return pltpu.make_async_remote_copy(
            src_ref=src_ref, dst_ref=dst_ref, send_sem=send.at[(out_dir, *at)], recv_sem=recv.at[(in_dir, *at)],
            device_id=to, device_id_type=MESH,
        )

    def x_lo_copy(t):
        return copy(ib.at[0, t], ir.at[1, t], {"gx": gx - 1}, (t, 0), X_LO, X_HI)

    def x_hi_copy(t):
        return copy(ib.at[1, t], ir.at[0, t], {"gx": gx + 1}, (t, 0), X_HI, X_LO)

    def y_copies(t, a):
        return (
            copy(jb.at[0, t, a], jr.at[1, t, a], {"gy": y_lo}, (t, a), Y_LO, Y_HI),
            copy(jb.at[1, t, a], jr.at[0, t, a], {"gy": y_hi}, (t, a), Y_HI, Y_LO),
        )

    def z_copies(t, a):
        up = copy(kb.at[t, a], kr.at[0, t, a], {"gz": z_hi}, (t, a), Z_HI, Z_LO)
        if one_z:
            return (up,)
        return (up, copy(kb.at[t, a], kr.at[1, t, a], {"gz": z_lo}, (t, a), Z_LO, Z_HI))

    def face(c, side):
        m = 1 if side == 0 else nm
        even = x[c, m, pl.ds(PAD, half, stride=2), :]
        odd = x[c, m, pl.ds(PAD + 1, half, stride=2), :]
        wanted = c if side == 0 else 1 - c
        return jnp.where(odd_lane_half, even, odd) if wanted == 1 else jnp.where(odd_lane_half, odd, even)

    def send_x(c, t):
        @pl.when(has_lo)
        def _():
            ib[0, t] = face(c, 0)
            x_lo_copy(t).start()

        @pl.when(has_hi)
        def _():
            ib[1, t] = face(c, 1)
            x_hi_copy(t).start()

    def send_z(t, a):
        for z in z_copies(t, a):
            z.start()

    def send_y(t, a, outermost):
        for h, m in enumerate((a, nm - 1 - a)):
            low, high = outermost(a, m, h)
            jb[0, t, a, pl.ds(h, 1), :] = low
            jb[1, t, a, pl.ds(h, 1), :] = high
        for y in y_copies(t, a):
            y.start()

    def take_yz(c, t, a):
        for z in z_copies(t, a):
            z.wait_recv()
        low = kr[0, t, a]
        high = low if one_z else kr[1, t, a]
        comb[a] = jnp.where(even_lane, pltpu.roll(high, cols - 1, 1), pltpu.roll(low, 1, 1))
        for y in y_copies(t, a):
            y.wait_recv()
        for h, m in enumerate((a, nm - 1 - a)):
            x[c, m + 1, pl.ds(PAD - 1, 1), :] = jr[0, t, a, pl.ds(h, 1), :]
            x[c, m + 1, pl.ds(PAD + rows, 1), :] = jr[1, t, a, pl.ds(h, 1), :]

    def take_x(c, t):
        @pl.when(has_lo)
        def _():
            x_hi_copy_in = copy(ib.at[1, t], ir.at[0, t], {"gx": gx - 1}, (t, 0), X_HI, X_LO)
            x_hi_copy_in.wait_recv()
            got = ir[0, t]
            x[c, 0, pl.ds(PAD, half, stride=2), :] = got
            x[c, 0, pl.ds(PAD + 1, half, stride=2), :] = got

        @pl.when(has_hi)
        def _():
            x_lo_copy_in = copy(ib.at[0, t], ir.at[1, t], {"gx": gx + 1}, (t, 0), X_LO, X_HI)
            x_lo_copy_in.wait_recv()
            got = ir[1, t]
            x[c, nm + 1, pl.ds(PAD, half, stride=2), :] = got
            x[c, nm + 1, pl.ds(PAD + 1, half, stride=2), :] = got

    def store_to(c):
        def store(m, start, y):
            x[c, m + 1, pl.ds(PAD + start, GROUP * 8), :] = flat(y)

        return store

    def black_of_field(a, m, q0, start):
        low = three(fv[2 * m, pl.ds(start, GROUP * 8), :])
        high = three(fv[2 * m + 1, pl.ds(start, GROUP * 8), :])
        return jnp.where(odd3, low, high)

    def pack_field(a, carry):
        for m in (a, nm - 1 - a):
            load(f_hbm, fv, fsem, m).wait()
        pair(black_of_field, store_to(1), a, kb.at[0])
        return carry

    def split_source(m, carry):
        for blk in range(per_plane // GROUP):
            rs = pl.ds(blk * GROUP * 8, GROUP * 8)
            low, high = three(sv[2 * m, rs, :]), three(sv[2 * m + 1, rs, :])
            src[0, m, rs, :] = flat(jnp.where(odd3, high, low))
            src[1, m, rs, :] = flat(jnp.where(odd3, low, high))
        return carry

    def split_pair(a, carry):
        for m in (a, nm - 1 - a):
            load(s_hbm, sv, ssem, m).wait()
            split_source(m, 0)
        return carry

    lax.fori_loop(0, nm // 2, pack_field, 0)
    lax.fori_loop(0, nm // 2, split_pair, 0)
    pl.semaphore_wait(barrier, len(ys) + len(zs) + has_lo.astype(jnp.int32) + has_hi.astype(jnp.int32))
    send_x(1, 0)

    def stored_rows(a, m, h):
        return x[1, m + 1, pl.ds(PAD, 1), :], x[1, m + 1, pl.ds(PAD + rows - 1, 1), :]

    for a in range(nm // 2):
        send_y(0, a, stored_rows)
        send_z(0, a)

    def relax(c, t):
        d = 1 - c

        def produce(a, m, q0, start):
            rs = pl.ds(PAD + start, GROUP * 8)
            here = three(x[d, m + 1, rs, :])
            below, above = three(x[d, m, rs, :]), three(x[d, m + 2, rs, :])
            beside = jnp.where(odd3, above, below) if c == 0 else jnp.where(odd3, below, above)
            total = three(src[c, m, pl.ds(start, GROUP * 8), :]) + here + beside
            total = total + three(x[d, m + 1, pl.ds(PAD + start - 1, GROUP * 8), :])
            total = total + three(x[d, m + 1, pl.ds(PAD + start + 1, GROUP * 8), :])
            edges = comb[a]
            edge = jnp.stack(
                [pltpu.roll(edges, (2 * cols - (2 * (q0 + g) + 1)) % cols, 1) for g in range(GROUP)], axis=0
            )
            total = total + jnp.where(first3, edge, pltpu.roll(here, 1, 2))
            total = total + jnp.where(last3, edge, pltpu.roll(here, cols - 1, 2))
            return total * jnp.float32(1.0 / 6.0)

        return produce

    def early_rows(c):
        d = 1 - c

        def tile(a, m, q, start):
            rs = pl.ds(PAD + start, 8)
            here = x[d, m + 1, rs, :]
            below, above = x[d, m, rs, :], x[d, m + 2, rs, :]
            beside = jnp.where(odd8 == 1, above, below) if c == 0 else jnp.where(odd8 == 1, below, above)
            total = src[c, m, pl.ds(start, 8), :] + here + beside
            total = total + x[d, m + 1, pl.ds(PAD + start - 1, 8), :]
            total = total + x[d, m + 1, pl.ds(PAD + start + 1, 8), :]
            edge = pltpu.roll(comb[a], (2 * cols - (2 * q + 1)) % cols, 1)
            total = total + jnp.where(lane == 0, edge, pltpu.roll(here, 1, 1))
            total = total + jnp.where(lane == cols - 1, edge, pltpu.roll(here, cols - 1, 1))
            return total * jnp.float32(1.0 / 6.0)

        def outermost(a, m, h):
            q = h * per_plane
            return tile(a, m, q, 0)[0:1], tile(a, m, q + per_plane - 1, rows - 8)[7:8]

        return outermost

    def store_out(m, start, y):
        red = three(x[0, m + 1, pl.ds(PAD + start, GROUP * 8), :])
        rs = pl.ds(start, GROUP * 8)
        ov[2 * m, rs, :] = flat(jnp.where(odd3, y, red))
        ov[2 * m + 1, rs, :] = flat(jnp.where(odd3, red, y))

    for t in range(rounds):
        c = t % 2
        final = t == rounds - 1
        store = store_out if final else store_to(c)
        pack = None if final else kb.at[t + 1]

        def piece(a, first=False):
            take_yz(1 - c, t, a)
            if first:
                take_x(1 - c, t)
            if not final:
                send_y(t + 1, a, early_rows(c))
            pair(relax(c, t), store, a, pack)
            if not final:
                if first:
                    send_x(c, t + 1)
                send_z(t + 1, a)

        def body(a, carry):
            piece(a)
            return carry

        piece(0, True)
        lax.fori_loop(1, nm // 2, body, 0)

    for t in range(rounds):
        for a in range(nm // 2):
            for cp in z_copies(t, a) + y_copies(t, a):
                cp.wait_send()

        @pl.when(has_lo)
        def _():
            x_lo_copy(t).wait_send()

        @pl.when(has_hi)
        def _():
            x_hi_copy(t).wait_send()


def solution(mesh):
    sizes = tuple(mesh.shape[a] for a in ("gx", "gy", "gz"))

    def on_device(field, source):
        planes, rows, cols = field.shape
        nm, rounds = planes // 2, 2 * SWEEPS
        assert planes % 4 == 0 and rows % (8 * GROUP) == 0 and cols == 128 and rows // 2 == cols
        f32 = jnp.float32
        return pl.pallas_call(
            functools.partial(kernel, sizes),
            out_shape=jax.ShapeDtypeStruct(field.shape, f32),
            in_specs=[pl.BlockSpec(memory_space=pltpu.HBM)] * 2,
            out_specs=pl.BlockSpec(memory_space=pltpu.VMEM),
            scratch_shapes=[
                pltpu.VMEM(field.shape, f32),
                pltpu.VMEM(field.shape, f32),
                pltpu.VMEM((2, nm + 2, rows + 2 * PAD, cols), f32),
                pltpu.VMEM((2, nm, rows, cols), f32),
                pltpu.VMEM((nm // 2, 8, cols), f32),
                pltpu.VMEM((rounds, nm // 2, 8, cols), f32),
                pltpu.VMEM((2, rounds, nm // 2, 8, cols), f32),
                pltpu.VMEM((2, rounds, nm // 2, 2, cols), f32),
                pltpu.VMEM((2, rounds, nm // 2, 2, cols), f32),
                pltpu.VMEM((2, rounds, rows // 2, cols), f32),
                pltpu.VMEM((2, rounds, rows // 2, cols), f32),
                pltpu.SemaphoreType.DMA((6, rounds, nm // 2)),
                pltpu.SemaphoreType.DMA((6, rounds, nm // 2)),
                pltpu.SemaphoreType.DMA((nm,)),
                pltpu.SemaphoreType.DMA((nm,)),
            ],
            compiler_params=pltpu.CompilerParams(
                collective_id=0, has_side_effects=True, vmem_limit_bytes=50 * 1024 * 1024
            ),
        )(field, source)

    spec = P("gx", "gy", "gz")
    return jax.shard_map(on_device, mesh=mesh, in_specs=(spec, spec), out_specs=spec, check_vma=False)
```
